32 devices in a mesh: grp: 2 (over y), seq: 8 (over z, x), tp: 2 (over core).
Axes of the slice: x: 2, y: 2, z: 4, core: 2. Of those that a mesh axis runs over, the one named last changes fastest.
Arguments:
- queries: bfloat16 [4096, 2048], P(('grp', 'seq'), 'tp'), parts along dimension 0, may hold values from -9 to 9
- keys: bfloat16 [4096, 2048], P(('grp', 'seq'), 'tp'), parts along dimension 0, may hold values from -9 to 9
- values: bfloat16 [4096, 2048], P(('grp', 'seq'), 'tp'), parts along dimension 0, may hold values from -18 to 18
- segment_ids: int32 [4096], P(('grp', 'seq')), parts along dimension 0, may hold values from 0 to 7, never falling along the last dimension, each value on 1 to 512 neighbouring positions
- modality: int32 [4096], P(('grp', 'seq')), parts along dimension 0, may hold values 0 or 1
- norm_gain: float32 [2, 2048], P(None, 'tp'), may hold values from 0.1 to 1.9
Outputs:
- blended: bfloat16 [4096, 2048], P(('grp', 'seq'), 'tp'), parts along dimension 0
The draws below stay inside these ranges and needn't reach their ends.
There are 2 independent parts, one for each index of `grp`. The reference program is written for one: setup_inputs(seed, part) draws one part's arguments, and reference() takes and returns one part's arrays. A program takes and returns all parts, laid end to end along the dimension named above; an argument that names none is the same for every part. Nothing has to cross between parts.
Inputs may be any that keep to these rules, and one draw needn't show every extreme that they name: `segment_ids`: ids never fall along the sequence; each document holds 1 to 512 tokens, and one holds exactly that many.
All inputs are finite; a program needn't handle non-finite values. No bound on the sum of `modality` on one device may be relied on, other than what follows from the above.
Results may differ from the reference program's by a relative error of at most 0.009.
Values may be sent and summed in bfloat16 or wider, within the bound.
A program may use at most 64 MiB of HBM per device.

```python
import math
import jax
import jax.numpy as jnp
import numpy as np
from jax import lax

HEADS = 16
HEAD_DIM = 128
TOK_DEV = 256
REACH = 2
TOKENS = 2048
DOCS = 8
N_SEQ = 8


def draw_entries(key, part):
    key_base = jax.random.fold_in(key, 7)
    key_query, key_other = jax.random.split(key_base, 2)
    array_shape = (TOKENS, HEADS * HEAD_DIM)
    query_draw = jnp.clip(jax.random.normal(key_query, array_shape, jnp.float32), -6.0, 6.0)
    key_draw = jnp.clip(jax.random.normal(key_other, array_shape, jnp.float32), -6.0, 6.0)
    return (query_draw, key_draw)


def draw_queries(key, part):
    return draw_entries(key, part)[0].astype(jnp.bfloat16)


def draw_keys(key, part):
    return draw_entries(key, part)[1].astype(jnp.bfloat16)


def draw_values(key, part):
    key_base = jax.random.fold_in(key, 11)
    key_entry, key_scale = jax.random.split(key_base, 2)
    array_shape = (TOKENS, HEADS * HEAD_DIM)
    entries = jnp.clip(jax.random.normal(key_entry, array_shape, jnp.float32), -6.0, 6.0)
    head_scale = jnp.exp(jax.random.uniform(key_scale, (HEADS,), jnp.float32, jnp.log(0.3), jnp.log(3.0)))
    column_scale = jnp.repeat(head_scale, HEAD_DIM)
    return (entries * column_scale[None, :]).astype(jnp.bfloat16)


def touch_ends(values, key, low, largest):
    place = [jax.random.randint(jax.random.fold_in(key, axis), (), 0, length) for axis, length in enumerate(values.shape)]
    main_axis = values.shape.index(max(values.shape))
    beside = place[:main_axis] + [(place[main_axis] + 1) % values.shape[main_axis]] + place[main_axis + 1:]
    return values.at[tuple(place)].set(low).at[tuple(beside)].set(largest)


def profile(number_of, total, limit, slope):
    weights = [(1 << 20) // math.isqrt(grade ** slope) + 1 for grade in range(2, number_of + 1)]
    spare, holding = total - limit - (number_of - 1), [1] * (number_of - 1)
    while spare > 0:
        candidates = [i for i in range(number_of - 1) if holding[i] < limit]
        pool, left = sum([weights[i] for i in candidates]), spare
        for i in candidates:
            extra = min(limit - holding[i], max(1, left * weights[i] // pool), spare)
            holding[i] = holding[i] + extra
            spare = spare - extra
    return np.array([limit] + holding)


def uneven(stream_key, count, total, bound, slope):
    if count == 2:
        one = jax.random.randint(stream_key, (), max(1, total - bound), min(bound, total - 1) + 1)
        return jnp.stack([one, total - one])
    tallies = jnp.asarray(profile(count, total, bound, slope), jnp.int32)
    pairs = (count - 1) // 2
    source_of, receiver = tallies[1:1 + 2 * pairs:2], tallies[2:2 + 2 * pairs:2]
    room = jnp.minimum(source_of - 1, bound - receiver)
    shifted = jax.random.randint(jax.random.fold_in(stream_key, 1), (pairs,), 0, 1 << 20) % (room + 1)
    tallies = tallies.at[1:1 + 2 * pairs:2].set(source_of - shifted).at[2:2 + 2 * pairs:2].set(receiver + shifted)
    return tallies[jax.random.permutation(jax.random.fold_in(stream_key, 2), count)]


def setup_inputs(seed: int = 0, part: int = 0) -> dict:
    streams_of = jax.random.split(jax.random.key(seed), 7)
    own_keys = jax.random.split(jax.random.fold_in(streams_of[6], part), 7)
    return {
        "queries": draw_queries(jax.random.fold_in(jax.random.fold_in(streams_of[6], part), 71), part),
        "keys": draw_keys(jax.random.fold_in(jax.random.fold_in(streams_of[6], part), 71), part),
        "values": draw_values(jax.random.fold_in(jax.random.fold_in(streams_of[6], part), 71), part),
        "segment_ids": jnp.searchsorted(jnp.cumsum(uneven(own_keys[3], DOCS, TOKENS, REACH * TOK_DEV, 1)), jnp.arange(TOKENS), side="right").astype(jnp.int32),
        "modality": touch_ends((jax.random.randint(own_keys[4], (TOKENS,), 0, 2) < 1).astype(jnp.int32), jax.random.fold_in(own_keys[4], 1), 0, 1),
        "norm_gain": jnp.clip(1.0 + 0.18 * jax.random.normal(streams_of[5], (2, HEADS * HEAD_DIM), jnp.float32), 0.1, 1.9),
    }


def attend_block(block_index, queries, keys, values, segment_ids):
    key_span = (REACH + 1) * TOK_DEV
    first_key = (jnp.maximum(block_index - REACH, 0) * TOK_DEV).astype(jnp.int32)
    first_query = (block_index * TOK_DEV).astype(jnp.int32)
    q_rows = lax.dynamic_slice_in_dim(queries, first_query, TOK_DEV, 0).astype(jnp.float32).reshape(TOK_DEV, HEADS, HEAD_DIM)
    k_rows = lax.dynamic_slice_in_dim(keys, first_key, key_span, 0).astype(jnp.float32).reshape(key_span, HEADS, HEAD_DIM)
    v_rows = lax.dynamic_slice_in_dim(values, first_key, key_span, 0).astype(jnp.float32).reshape(key_span, HEADS, HEAD_DIM)
    query_segs = lax.dynamic_slice_in_dim(segment_ids, first_query, TOK_DEV, 0)
    key_segs = lax.dynamic_slice_in_dim(segment_ids, first_key, key_span, 0)
    query_pos = first_query + jnp.arange(TOK_DEV, dtype=jnp.int32)
    key_pos = first_key + jnp.arange(key_span, dtype=jnp.int32)
    allowed = (query_segs[:, None] == key_segs[None, :]) & (key_pos[None, :] <= query_pos[:, None])
    scores = jnp.einsum('qhd,khd->hqk', q_rows, k_rows) * HEAD_DIM ** (-0.5)
    scores = jnp.where(allowed[None], scores, -jnp.inf)
    row_max = lax.optimization_barrier(jnp.max(scores, axis=2, keepdims=True))
    weights = jnp.exp(scores - row_max)
    row_total = lax.optimization_barrier(jnp.sum(weights, axis=2))
    rounded = weights.astype(jnp.bfloat16).astype(jnp.float32)
    summed = jnp.einsum('hqk,khd->qhd', rounded, v_rows)
    attended = summed / jnp.transpose(row_total)[:, :, None]
    return attended.reshape(TOK_DEV, HEADS * HEAD_DIM).astype(jnp.bfloat16)

def reference(queries, keys, values, segment_ids, modality, norm_gain):
    indices = jnp.arange(N_SEQ, dtype=jnp.int32)
    attended = lax.map(lambda block_index: attend_block(block_index, queries, keys, values, segment_ids), indices)
    attended = attended.reshape(TOKENS, HEADS * HEAD_DIM).astype(jnp.float32)
    mean_square = lax.optimization_barrier(jnp.sum(attended * attended, axis=1)) / (HEADS * HEAD_DIM)
    gain_rows = jnp.where((modality == 1)[:, None], norm_gain[1][None, :], norm_gain[0][None, :])
    blended = attended * lax.rsqrt(mean_square + 1e-05)[:, None] * gain_rows
    return blended.astype(jnp.bfloat16)
```

```python
import functools

import jax
import jax.numpy as jnp
from jax import lax
from jax.experimental import pallas as pl
from jax.experimental.pallas import tpu as pltpu
from jax.sharding import PartitionSpec as P

HEADS = 16
HEAD_DIM = 128
REACH = 2
MESH = pl.DeviceIdType.MESH


def kernel(
    n,
    heads,
    rows,
    q_hbm,
    k_hbm,
    v_hbm,
    seg_ref,
    mod_ref,
    gain_ref,
    out_ref,
    q_own,
    own,
    buf1,
    buf2,
    seg1,
    seg2,
    bias,
    att,
    squares,
    mine,
    theirs,
    in_sem,
    send_a,
    send_b,
    send_c,
    recv_1,
    recv_2,
    seg_send,
    seg_recv,
    sq_sem,
):
    s = lax.axis_index("seq")
    t = lax.axis_index("tp")
    even = lax.rem(s, 2) == 0
    odd = lax.rem(s, 2) == 1
    has_next = s + 2 < n
    has_prev = s >= 2
    pair = s + 1 - 2 * lax.rem(s, 2)

    def load(source, target, h, j):
        columns = pl.ds(h * HEAD_DIM, HEAD_DIM)
        return pltpu.make_async_copy(source.at[:, columns], target, in_sem.at[h, j])

    def load_k(h):
        return load(k_hbm, own.at[h, 0], h, 0)

    def load_v(h):
        return load(v_hbm, own.at[h, 1], h, 1)

    def load_q(h):
        return load(q_hbm, q_own.at[h], h, 2)

    for h in range(heads):
        load_k(h).start()
        load_v(h).start()

    barrier = pltpu.get_barrier_semaphore()
    pl.semaphore_signal(barrier, inc=1, device_id={"tp": 1 - t}, device_id_type=MESH)
    pl.semaphore_signal(barrier, inc=1, device_id={"seq": pair}, device_id_type=MESH)

    @pl.when(has_next)
    def _():
        pl.semaphore_signal(barrier, inc=1, device_id={"seq": s + 2}, device_id_type=MESH)

    @pl.when(has_prev)
    def _():
        pl.semaphore_signal(barrier, inc=1, device_id={"seq": s - 2}, device_id_type=MESH)

    peers = 2 + jnp.where(has_next, 1, 0) + jnp.where(has_prev, 1, 0)
    pl.semaphore_wait(barrier, peers)

    def remote(source, target, send, recv, where):
        return pltpu.make_async_remote_copy(
            src_ref=source,
            dst_ref=target,
            send_sem=send,
            recv_sem=recv,
            device_id={"seq": where},
            device_id_type=MESH,
        )

    def flow_a(h):
        return remote(own.at[h], buf1.at[h], send_a.at[h], recv_1.at[h], pair)

    def flow_b(h):
        return remote(own.at[h], buf2.at[h], send_b.at[h], recv_2.at[h], s + 2)

    def flow_c(h):
        return remote(buf2.at[h], buf1.at[h], send_c.at[h], recv_1.at[h], pair)

    def seg_a():
        return remote(seg_ref, seg1, seg_send.at[0], seg_recv.at[0], pair)

    def seg_b():
        return remote(seg_ref, seg2, seg_send.at[1], seg_recv.at[1], s + 2)

    def seg_c():
        return remote(seg2, seg1, seg_send.at[2], seg_recv.at[0], pair)

    @pl.when(even)
    def _():
        seg_a().start()

    @pl.when(has_next)
    def _():
        seg_b().start()

    def send(h, carry):
        load_k(h).wait()
        load_v(h).wait()

        @pl.when(has_next)
        def _():
            flow_b(h).start()

        @pl.when(even)
        def _():
            flow_a(h).start()

        load_q(h).start()
        return carry

    lax.fori_loop(0, heads, send, 0)

    @pl.when(s < 1)
    def _():
        buf1[...] = jnp.zeros_like(buf1)
        seg1[...] = jnp.full_like(seg1, -1)

    @pl.when(s < 2)
    def _():
        buf2[...] = jnp.zeros_like(buf2)
        seg2[...] = jnp.full_like(seg2, -1)

    def column(row):
        return jnp.transpose(jnp.broadcast_to(row, (HEAD_DIM, rows)))

    query_seg = column(seg_ref[...])[:, :1]
    query_pos = lax.broadcasted_iota(jnp.int32, (rows, rows), 0)
    key_pos = lax.broadcasted_iota(jnp.int32, (rows, rows), 1)
    allowed = (query_seg == seg_ref[...]) & (key_pos <= query_pos)
    bias[:, :rows] = jnp.where(allowed, 0.0, -jnp.inf)
    squares[...] = jnp.zeros_like(squares)

    @pl.when(has_prev)
    def _():
        seg_b().wait_recv()

    @pl.when(odd & has_prev)
    def _():
        seg_c().start()

    @pl.when(s >= 1)
    def _():
        seg_a().wait_recv()

    bias[:, rows : 2 * rows] = jnp.where(query_seg == seg1[...], 0.0, -jnp.inf)
    bias[:, 2 * rows :] = jnp.where(query_seg == seg2[...], 0.0, -jnp.inf)

    def scores_of(query, key):
        return lax.dot_general(
            query, key, (((1,), (1,)), ((), ())), preferred_element_type=jnp.float32
        )

    def head(h, carry):
        load_q(h).wait()

        @pl.when(has_prev)
        def _():
            flow_b(h).wait_recv()

        @pl.when(odd & has_prev)
        def _():
            flow_c(h).start()

        @pl.when(s >= 1)
        def _():
            flow_a(h).wait_recv()

        query = q_own[h]
        scale = HEAD_DIM ** (-0.5)
        blocks = (own, buf1, buf2)
        scores = [
            scores_of(query, block[h, 0]) * scale + bias[:, i * rows : (i + 1) * rows]
            for i, block in enumerate(blocks)
        ]
        top = jnp.maximum(jnp.maximum(scores[0], scores[1]), scores[2])
        top = jnp.max(top, axis=1, keepdims=True)
        weights = [jnp.exp(score - top) for score in scores]
        total = jnp.sum(weights[0] + weights[1] + weights[2], axis=1, keepdims=True)
        acc = jnp.zeros((rows, HEAD_DIM), jnp.float32)
        for weight, block in zip(weights, blocks):
            acc = acc + jnp.dot(
                weight.astype(jnp.bfloat16), block[h, 1], preferred_element_type=jnp.float32
            )
        attended = (acc * (1.0 / total)).astype(jnp.bfloat16)
        att[h] = attended
        wide = attended.astype(jnp.float32)
        squares[...] += wide * wide
        return carry

    lax.fori_loop(0, heads, head, 0)

    partial = jnp.sum(squares[...], axis=1, keepdims=True)
    mine[...] = jnp.broadcast_to(partial, mine.shape)
    swap = pltpu.make_async_remote_copy(
        src_ref=mine,
        dst_ref=theirs,
        send_sem=sq_sem.at[0],
        recv_sem=sq_sem.at[1],
        device_id={"tp": 1 - t},
        device_id_type=MESH,
    )
    swap.start()
    image = column(mod_ref[...]) == 1
    swap.wait_recv()
    mean_square = (mine[...] + theirs[...]) / (HEADS * HEAD_DIM)
    inverse = lax.rsqrt(mean_square + 1e-05)
    for h in range(heads):
        columns = slice(h * HEAD_DIM, (h + 1) * HEAD_DIM)
        gain = jnp.where(image, gain_ref[1:2, columns], gain_ref[0:1, columns])
        out_ref[:, columns] = (att[h].astype(jnp.float32) * inverse * gain).astype(out_ref.dtype)

    swap.wait_send()

    @pl.when(even)
    def _():
        seg_a().wait_send()

    @pl.when(has_next)
    def _():
        seg_b().wait_send()

    @pl.when(odd & has_prev)
    def _():
        seg_c().wait_send()

    def drain(h, carry):
        @pl.when(even)
        def _():
            flow_a(h).wait_send()

        @pl.when(has_next)
        def _():
            flow_b(h).wait_send()

        @pl.when(odd & has_prev)
        def _():
            flow_c(h).wait_send()

        return carry

    lax.fori_loop(0, heads, drain, 0)


def on_device(n, queries, keys, values, segment_ids, modality, norm_gain):
    rows, width = queries.shape
    heads = width // HEAD_DIM
    vmem = pl.BlockSpec(memory_space=pltpu.VMEM)
    hbm = pl.BlockSpec(memory_space=pl.ANY)
    block = pltpu.VMEM((heads, 2, rows, HEAD_DIM), jnp.bfloat16)
    return pl.pallas_call(
        functools.partial(kernel, n, heads, rows),
        out_shape=jax.ShapeDtypeStruct((rows, width), jnp.bfloat16),
        in_specs=[hbm, hbm, hbm, vmem, vmem, vmem],
        out_specs=vmem,
        scratch_shapes=[
            pltpu.VMEM((heads, rows, HEAD_DIM), jnp.bfloat16),
            block,
            block,
            block,
            pltpu.VMEM((1, rows), jnp.int32),
            pltpu.VMEM((1, rows), jnp.int32),
            pltpu.VMEM((rows, (REACH + 1) * rows), jnp.float32),
            pltpu.VMEM((heads, rows, HEAD_DIM), jnp.bfloat16),
            pltpu.VMEM((rows, HEAD_DIM), jnp.float32),
            pltpu.VMEM((rows, HEAD_DIM), jnp.float32),
            pltpu.VMEM((rows, HEAD_DIM), jnp.float32),
            pltpu.SemaphoreType.DMA((heads, 3)),
            pltpu.SemaphoreType.DMA((heads,)),
            pltpu.SemaphoreType.DMA((heads,)),
            pltpu.SemaphoreType.DMA((heads,)),
            pltpu.SemaphoreType.DMA((heads,)),
            pltpu.SemaphoreType.DMA((heads,)),
            pltpu.SemaphoreType.DMA((3,)),
            pltpu.SemaphoreType.DMA((2,)),
            pltpu.SemaphoreType.DMA((2,)),
        ],
        compiler_params=pltpu.CompilerParams(collective_id=0, has_side_effects=True),
    )(
        queries,
        keys,
        values,
        segment_ids.reshape(1, rows),
        modality.reshape(1, rows),
        norm_gain,
    )


def solution(mesh):
    return jax.shard_map(
        functools.partial(on_device, mesh.shape["seq"]),
        mesh=mesh,
        in_specs=(
            P(("grp", "seq"), "tp"),
            P(("grp", "seq"), "tp"),
            P(("grp", "seq"), "tp"),
            P(("grp", "seq")),
            P(("grp", "seq")),
            P(None, "tp"),
        ),
        out_specs=P(("grp", "seq"), "tp"),
        check_vma=False,
    )
```

```python
import functools

import jax
import jax.numpy as jnp
from jax import lax
from jax.experimental import pallas as pl
from jax.experimental.pallas import tpu as pltpu
from jax.sharding import PartitionSpec as P

HEADS = 16
HEAD_DIM = 128
REACH = 2
MESH = pl.DeviceIdType.MESH
PIECES = 4


def kernel(
    n,
    heads,
    rows,
    q_hbm,
    k_hbm,
    v_hbm,
    seg_ref,
    mod_ref,
    att,
    inverse_ref,
    image_ref,
    q_own,
    own,
    buf1,
    buf2,
    seg1,
    seg2,
    bias,
    squares,
    mine,
    theirs,
    in_sem,
    send_a,
    send_b,
    send_c,
    recv_1,
    recv_2,
    seg_send,
    seg_recv,
    sq_sem,
):
    s = lax.axis_index("seq")
    t = lax.axis_index("tp")
    even = lax.rem(s, 2) == 0
    odd = lax.rem(s, 2) == 1
    has_next = s + 2 < n
    has_prev = s >= 2
    pair = s + 1 - 2 * lax.rem(s, 2)

    half = PIECES // 2
    depth = rows // half

    def columns_of(h):
        return pl.ds(h * HEAD_DIM, HEAD_DIM)

    def load_piece(h, p):
        source = k_hbm if p < half else v_hbm
        piece = pl.ds((p % half) * depth, depth)
        return pltpu.make_async_copy(
            source.at[piece, columns_of(h)], own.at[h, p], in_sem.at[h, p]
        )

    def load_q(h):
        return pltpu.make_async_copy(q_hbm.at[:, columns_of(h)], q_own.at[h], in_sem.at[h, PIECES])

    for h in range(heads):
        for p in range(PIECES):
            load_piece(h, p).start()

    barrier = pltpu.get_barrier_semaphore()
    pl.semaphore_signal(barrier, inc=1, device_id={"tp": 1 - t}, device_id_type=MESH)
    pl.semaphore_signal(barrier, inc=1, device_id={"seq": pair}, device_id_type=MESH)

    @pl.when(has_next)
    def _():
        pl.semaphore_signal(barrier, inc=1, device_id={"seq": s + 2}, device_id_type=MESH)

    @pl.when(has_prev)
    def _():
        pl.semaphore_signal(barrier, inc=1, device_id={"seq": s - 2}, device_id_type=MESH)

    peers = 2 + jnp.where(has_next, 1, 0) + jnp.where(has_prev, 1, 0)
    pl.semaphore_wait(barrier, peers)

    def remote(source, target, send, recv, where):
        return pltpu.make_async_remote_copy(
            src_ref=source,
            dst_ref=target,
            send_sem=send,
            recv_sem=recv,
            device_id={"seq": where},
            device_id_type=MESH,
        )

    def flow_a(h, p):
        return remote(own.at[h, p], buf1.at[h, p], send_a.at[h, p], recv_1.at[h, p], pair)

    def flow_b(h, p):
        return remote(own.at[h, p], buf2.at[h, p], send_b.at[h, p], recv_2.at[h, p], s + 2)

    def flow_c(h, p):
        return remote(buf2.at[h, p], buf1.at[h, p], send_c.at[h, p], recv_1.at[h, p], pair)

    def seg_a():
        return remote(seg_ref, seg1, seg_send.at[0], seg_recv.at[0], pair)

    def seg_b():
        return remote(seg_ref, seg2, seg_send.at[1], seg_recv.at[1], s + 2)

    def seg_c():
        return remote(seg2, seg1, seg_send.at[2], seg_recv.at[0], pair)

    @pl.when(even)
    def _():
        seg_a().start()

    @pl.when(has_next)
    def _():
        seg_b().start()

    def send(h, carry):
        for p in range(PIECES):
            load_piece(h, p).wait()

            @pl.when(has_next)
            def _():
                flow_b(h, p).start()

            @pl.when(even)
            def _():
                flow_a(h, p).start()

        load_q(h).start()
        return carry

    lax.fori_loop(0, heads, send, 0)

    @pl.when(s < 1)
    def _():
        buf1[...] = jnp.zeros_like(buf1)
        seg1[...] = jnp.full_like(seg1, -1)

    @pl.when(s < 2)
    def _():
        buf2[...] = jnp.zeros_like(buf2)
        seg2[...] = jnp.full_like(seg2, -1)

    def column(row):
        return jnp.transpose(jnp.broadcast_to(row, (HEAD_DIM, rows)))

    query_seg = column(seg_ref[...])[:, :1]
    query_pos = lax.broadcasted_iota(jnp.int32, (rows, rows), 0)
    key_pos = lax.broadcasted_iota(jnp.int32, (rows, rows), 1)
    allowed = (query_seg == seg_ref[...]) & (key_pos <= query_pos)
    bias[:, :rows] = jnp.where(allowed, 0.0, -jnp.inf)
    squares[...] = jnp.zeros_like(squares)
    image_ref[...] = column(mod_ref[...])

    @pl.when(has_prev)
    def _():
        seg_b().wait_recv()

    @pl.when(odd & has_prev)
    def _():
        seg_c().start()

    @pl.when(s >= 1)
    def _():
        seg_a().wait_recv()

    bias[:, rows : 2 * rows] = jnp.where(query_seg == seg1[...], 0.0, -jnp.inf)
    bias[:, 2 * rows :] = jnp.where(query_seg == seg2[...], 0.0, -jnp.inf)

    def scores_of(query, key):
        return lax.dot_general(
            query, key, (((1,), (1,)), ((), ())), preferred_element_type=jnp.float32
        )

    def arrive(h, pieces):
        for p in pieces:

            @pl.when(s >= 1)
            def _():
                flow_a(h, p).wait_recv()

    def head(h, carry):
        load_q(h).wait()
        query = q_own[h]
        scale = HEAD_DIM ** (-0.5)

        def scores_with(block, i):
            key = block[h, :half].reshape(rows, HEAD_DIM)
            return scores_of(query, key) * scale + bias[:, i * rows : (i + 1) * rows]

        def product(weight, block):
            value = block[h, half:].reshape(rows, HEAD_DIM)
            return jnp.dot(
                weight.astype(jnp.bfloat16), value, preferred_element_type=jnp.float32
            )

        for p in range(PIECES):

            @pl.when(has_prev)
            def _():
                flow_b(h, p).wait_recv()

            @pl.when(odd & has_prev)
            def _():
                flow_c(h, p).start()

        near = scores_with(own, 0)
        far = scores_with(buf2, 2)
        arrive(h, range(half))
        middle = scores_with(buf1, 1)
        top = jnp.max(jnp.maximum(jnp.maximum(near, middle), far), axis=1, keepdims=True)
        near = jnp.exp(near - top)
        far = jnp.exp(far - top)
        middle = jnp.exp(middle - top)
        total = jnp.sum(near + middle + far, axis=1, keepdims=True)
        acc = product(near, own) + product(far, buf2)
        arrive(h, range(half, PIECES))
        acc = acc + product(middle, buf1)
        attended = (acc * (1.0 / total)).astype(jnp.bfloat16)
        att[h] = attended
        wide = attended.astype(jnp.float32)
        squares[...] += wide * wide
        return carry

    lax.fori_loop(0, heads, head, 0)

    partial = jnp.sum(squares[...], axis=1, keepdims=True)
    mine[...] = jnp.broadcast_to(partial, mine.shape)
    swap = pltpu.make_async_remote_copy(
        src_ref=mine,
        dst_ref=theirs,
        send_sem=sq_sem.at[0],
        recv_sem=sq_sem.at[1],
        device_id={"tp": 1 - t},
        device_id_type=MESH,
    )
    swap.start()
    swap.wait_recv()
    mean_square = (mine[...] + theirs[...]) / (HEADS * HEAD_DIM)
    inverse_ref[...] = lax.rsqrt(mean_square + 1e-05)
    swap.wait_send()

    @pl.when(even)
    def _():
        seg_a().wait_send()

    @pl.when(has_next)
    def _():
        seg_b().wait_send()

    @pl.when(odd & has_prev)
    def _():
        seg_c().wait_send()

    def drain(h, carry):
        for p in range(PIECES):

            @pl.when(even)
            def _():
                flow_a(h, p).wait_send()

            @pl.when(has_next)
            def _():
                flow_b(h, p).wait_send()

            @pl.when(odd & has_prev)
            def _():
                flow_c(h, p).wait_send()

        return carry

    lax.fori_loop(0, heads, drain, 0)


def blend(heads, att, inverse_ref, image_ref, gain_ref, out_hbm, staged, out_sem):
    inverse = inverse_ref[...]
    image = image_ref[...] == 1
    copies = []
    for h in range(heads):
        columns = slice(h * HEAD_DIM, (h + 1) * HEAD_DIM)
        gain = jnp.where(image, gain_ref[1:2, columns], gain_ref[0:1, columns])
        staged[h] = (att[h].astype(jnp.float32) * inverse * gain).astype(staged.dtype)
        copy = pltpu.make_async_copy(
            staged.at[h], out_hbm.at[:, pl.ds(h * HEAD_DIM, HEAD_DIM)], out_sem.at[h]
        )
        copy.start()
        copies.append(copy)
    for copy in copies:
        copy.wait()


def on_device(n, queries, keys, values, segment_ids, modality, norm_gain):
    rows, width = queries.shape
    heads = width // HEAD_DIM
    vmem = pl.BlockSpec(memory_space=pltpu.VMEM)
    hbm = pl.BlockSpec(memory_space=pltpu.HBM)
    depth = 2 * rows // PIECES
    block = pltpu.VMEM((heads, PIECES, depth, HEAD_DIM), jnp.bfloat16)
    flow = pltpu.SemaphoreType.DMA((heads, PIECES))
    att, inverse, image = pl.pallas_call(
        functools.partial(kernel, n, heads, rows),
        out_shape=(
            pltpu.VMEM((heads, rows, HEAD_DIM), jnp.bfloat16),
            pltpu.VMEM((rows, HEAD_DIM), jnp.float32),
            pltpu.VMEM((rows, HEAD_DIM), jnp.int32),
        ),
        in_specs=[hbm, hbm, hbm, vmem, vmem],
        out_specs=(vmem, vmem, vmem),
        scratch_shapes=[
            pltpu.VMEM((heads, rows, HEAD_DIM), jnp.bfloat16),
            block,
            block,
            block,
            pltpu.VMEM((1, rows), jnp.int32),
            pltpu.VMEM((1, rows), jnp.int32),
            pltpu.VMEM((rows, (REACH + 1) * rows), jnp.float32),
            pltpu.VMEM((rows, HEAD_DIM), jnp.float32),
            pltpu.VMEM((rows, HEAD_DIM), jnp.float32),
            pltpu.VMEM((rows, HEAD_DIM), jnp.float32),
            pltpu.SemaphoreType.DMA((heads, PIECES + 1)),
            flow,
            flow,
            flow,
            flow,
            flow,
            pltpu.SemaphoreType.DMA((3,)),
            pltpu.SemaphoreType.DMA((2,)),
            pltpu.SemaphoreType.DMA((2,)),
        ],
        compiler_params=pltpu.CompilerParams(
            collective_id=0, has_side_effects=True
        ),
    )(queries, keys, values, segment_ids.reshape(1, rows), modality.reshape(1, rows))
    return pl.pallas_call(
        functools.partial(blend, heads),
        out_shape=jax.ShapeDtypeStruct((rows, width), jnp.bfloat16),
        in_specs=[vmem, vmem, vmem, vmem],
        out_specs=hbm,
        scratch_shapes=[
            pltpu.VMEM((heads, rows, HEAD_DIM), jnp.bfloat16),
            pltpu.SemaphoreType.DMA((heads,)),
        ],
        compiler_params=pltpu.CompilerParams(vmem_limit_bytes=8 * 2**20),
    )(att, inverse, image, norm_gain)


def solution(mesh):
    return jax.shard_map(
        functools.partial(on_device, mesh.shape["seq"]),
        mesh=mesh,
        in_specs=(
            P(("grp", "seq"), "tp"),
            P(("grp", "seq"), "tp"),
            P(("grp", "seq"), "tp"),
            P(("grp", "seq")),
            P(("grp", "seq")),
            P(None, "tp"),
        ),
        out_specs=P(("grp", "seq"), "tp"),
        check_vma=False,
    )
```

```python
import functools

import jax
import jax.numpy as jnp
from jax import lax
from jax.experimental import pallas as pl
from jax.experimental.pallas import tpu as pltpu
from jax.sharding import PartitionSpec as P

HEADS = 16
HEAD_DIM = 128
REACH = 2
MESH = pl.DeviceIdType.MESH
PIECES = 4
DIRECT = 2


def kernel(
    n,
    heads,
    rows,
    q_hbm,
    k_hbm,
    v_hbm,
    seg_ref,
    mod_ref,
    att,
    inverse_ref,
    image_ref,
    q_own,
    own,
    buf1,
    buf2,
    seg1,
    seg2,
    bias,
    squares,
    mine,
    theirs,
    in_sem,
    send_a,
    send_b,
    send_c,
    recv_1,
    recv_2,
    seg_send,
    seg_recv,
    sq_sem,
):
    s = lax.axis_index("seq")
    t = lax.axis_index("tp")
    even = lax.rem(s, 2) == 0
    odd = lax.rem(s, 2) == 1
    has_next = s + 2 < n
    has_prev = s >= 2
    pair = s + 1 - 2 * lax.rem(s, 2)

    half = PIECES // 2
    depth = rows // half

    def columns_of(h):
        return pl.ds(h * HEAD_DIM, HEAD_DIM)

    def load_piece(h, p):
        source = k_hbm if p < half else v_hbm
        piece = pl.ds((p % half) * depth, depth)
        return pltpu.make_async_copy(
            source.at[piece, columns_of(h)], own.at[h, p], in_sem.at[h, p]
        )

    def load_q(h):
        return pltpu.make_async_copy(q_hbm.at[:, columns_of(h)], q_own.at[h], in_sem.at[h, PIECES])

    last = heads - 1
    direct = range(PIECES - DIRECT, PIECES)
    for p in direct:
        load_piece(last, p).start()
    for h in range(heads):
        for p in range(PIECES):
            if h < last or p not in direct:
                load_piece(h, p).start()

    barrier = pltpu.get_barrier_semaphore()
    pl.semaphore_signal(barrier, inc=1, device_id={"tp": 1 - t}, device_id_type=MESH)
    pl.semaphore_signal(barrier, inc=1, device_id={"seq": pair}, device_id_type=MESH)

    @pl.when(has_next)
    def _():
        pl.semaphore_signal(barrier, inc=1, device_id={"seq": s + 2}, device_id_type=MESH)

    @pl.when(has_prev)
    def _():
        pl.semaphore_signal(barrier, inc=1, device_id={"seq": s - 2}, device_id_type=MESH)

    ahead = odd & (s + 1 < n)
    behind = even & has_prev

    @pl.when(ahead)
    def _():
        pl.semaphore_signal(barrier, inc=1, device_id={"seq": s + 1}, device_id_type=MESH)

    @pl.when(behind)
    def _():
        pl.semaphore_signal(barrier, inc=1, device_id={"seq": s - 1}, device_id_type=MESH)

    peers = jnp.where(ahead, 1, 0) + jnp.where(behind, 1, 0) + 2 + jnp.where(has_next, 1, 0) + jnp.where(has_prev, 1, 0)
    pl.semaphore_wait(barrier, peers)

    def remote(source, target, send, recv, where):
        return pltpu.make_async_remote_copy(
            src_ref=source,
            dst_ref=target,
            send_sem=send,
            recv_sem=recv,
            device_id={"seq": where},
            device_id_type=MESH,
        )

    def flow_a(h, p):
        return remote(own.at[h, p], buf1.at[h, p], send_a.at[h, p], recv_1.at[h, p], pair)

    def flow_b(h, p):
        return remote(own.at[h, p], buf2.at[h, p], send_b.at[h, p], recv_2.at[h, p], s + 2)

    def flow_c(h, p):
        return remote(buf2.at[h, p], buf1.at[h, p], send_c.at[h, p], recv_1.at[h, p], pair)

    def flow_d(p):
        return remote(
            own.at[last, p], buf1.at[last, p], send_c.at[last, p], recv_1.at[last, p], s + 1
        )

    def forwards(h, p):
        return odd & has_prev & (h < last) if p in direct else odd & has_prev

    def seg_a():
        return remote(seg_ref, seg1, seg_send.at[0], seg_recv.at[0], pair)

    def seg_b():
        return remote(seg_ref, seg2, seg_send.at[1], seg_recv.at[1], s + 2)

    def seg_c():
        return remote(seg2, seg1, seg_send.at[2], seg_recv.at[0], pair)

    @pl.when(even)
    def _():
        seg_a().start()

    @pl.when(has_next)
    def _():
        seg_b().start()

    for p in direct:
        load_piece(last, p).wait()

        @pl.when(ahead)
        def _():
            flow_d(p).start()

    def send_pieces(h, waits):
        for p in range(PIECES):
            if p in waits:
                load_piece(h, p).wait()

            @pl.when(has_next)
            def _():
                flow_b(h, p).start()

            @pl.when(even)
            def _():
                flow_a(h, p).start()

        load_q(h).start()

    def send(h, carry):
        send_pieces(h, range(PIECES))
        return carry

    lax.fori_loop(0, last, send, 0)
    send_pieces(last, range(PIECES - DIRECT))

    @pl.when(s < 1)
    def _():
        buf1[...] = jnp.zeros_like(buf1)
        seg1[...] = jnp.full_like(seg1, -1)

    @pl.when(s < 2)
    def _():
        buf2[...] = jnp.zeros_like(buf2)
        seg2[...] = jnp.full_like(seg2, -1)

    def column(row):
        return jnp.transpose(jnp.broadcast_to(row, (HEAD_DIM, rows)))

    query_seg = column(seg_ref[...])[:, :1]
    query_pos = lax.broadcasted_iota(jnp.int32, (rows, rows), 0)
    key_pos = lax.broadcasted_iota(jnp.int32, (rows, rows), 1)
    allowed = (query_seg == seg_ref[...]) & (key_pos <= query_pos)
    bias[:, :rows] = jnp.where(allowed, 0.0, -jnp.inf)
    squares[...] = jnp.zeros_like(squares)
    image_ref[...] = column(mod_ref[...])

    @pl.when(has_prev)
    def _():
        seg_b().wait_recv()

    @pl.when(odd & has_prev)
    def _():
        seg_c().start()

    @pl.when(s >= 1)
    def _():
        seg_a().wait_recv()

    bias[:, rows : 2 * rows] = jnp.where(query_seg == seg1[...], 0.0, -jnp.inf)
    bias[:, 2 * rows :] = jnp.where(query_seg == seg2[...], 0.0, -jnp.inf)

    def scores_of(query, key):
        return lax.dot_general(
            query, key, (((1,), (1,)), ((), ())), preferred_element_type=jnp.float32
        )

    def arrive(h, pieces):
        for p in pieces:

            @pl.when(s >= 1)
            def _():
                flow_a(h, p).wait_recv()

    def head(h, carry):
        load_q(h).wait()
        query = q_own[h]
        scale = HEAD_DIM ** (-0.5)

        def scores_with(block, i):
            key = block[h, :half].reshape(rows, HEAD_DIM)
            return scores_of(query, key) * scale + bias[:, i * rows : (i + 1) * rows]

        def product(weight, block):
            value = block[h, half:].reshape(rows, HEAD_DIM)
            return jnp.dot(
                weight.astype(jnp.bfloat16), value, preferred_element_type=jnp.float32
            )

        for p in range(half):

            @pl.when(has_prev)
            def _():
                flow_b(h, p).wait_recv()

            @pl.when(forwards(h, p))
            def _():
                flow_c(h, p).start()

        @pl.when(odd & has_prev)
        def _():
            for p in range(half, PIECES):
                flow_b(h, p).wait_recv()

                @pl.when(forwards(h, p))
                def _():
                    flow_c(h, p).start()

        near = scores_with(own, 0)
        far = scores_with(buf2, 2)
        arrive(h, range(half))
        middle = scores_with(buf1, 1)
        top = jnp.max(jnp.maximum(jnp.maximum(near, middle), far), axis=1, keepdims=True)
        near = jnp.exp(near - top)
        far = jnp.exp(far - top)
        middle = jnp.exp(middle - top)
        total = jnp.sum(near + middle + far, axis=1, keepdims=True)
        acc = product(near, own)

        @pl.when(behind)
        def _():
            for p in range(half, PIECES):
                flow_b(h, p).wait_recv()

        arrive(h, range(half, PIECES))
        acc = acc + product(far, buf2) + product(middle, buf1)
        attended = (acc * (1.0 / total)).astype(jnp.bfloat16)
        att[h] = attended
        wide = attended.astype(jnp.float32)
        squares[...] += wide * wide
        return carry

    lax.fori_loop(0, heads, head, 0)

    partial = jnp.sum(squares[...], axis=1, keepdims=True)
    mine[...] = jnp.broadcast_to(partial, mine.shape)
    swap = pltpu.make_async_remote_copy(
        src_ref=mine,
        dst_ref=theirs,
        send_sem=sq_sem.at[0],
        recv_sem=sq_sem.at[1],
        device_id={"tp": 1 - t},
        device_id_type=MESH,
    )
    swap.start()
    swap.wait_recv()
    mean_square = (mine[...] + theirs[...]) / (HEADS * HEAD_DIM)
    inverse_ref[...] = lax.rsqrt(mean_square + 1e-05)
    swap.wait_send()

    for p in direct:

        @pl.when(ahead)
        def _():
            flow_d(p).wait_send()

    @pl.when(even)
    def _():
        seg_a().wait_send()

    @pl.when(has_next)
    def _():
        seg_b().wait_send()

    @pl.when(odd & has_prev)
    def _():
        seg_c().wait_send()

    def drain(h, carry):
        for p in range(PIECES):

            @pl.when(even)
            def _():
                flow_a(h, p).wait_send()

            @pl.when(has_next)
            def _():
                flow_b(h, p).wait_send()

            @pl.when(forwards(h, p))
            def _():
                flow_c(h, p).wait_send()

        return carry

    lax.fori_loop(0, heads, drain, 0)


def blend(heads, att, inverse_ref, image_ref, gain_ref, out_hbm, staged, out_sem):
    inverse = inverse_ref[...]
    image = image_ref[...] == 1
    copies = []
    for h in range(heads):
        columns = slice(h * HEAD_DIM, (h + 1) * HEAD_DIM)
        gain = jnp.where(image, gain_ref[1:2, columns], gain_ref[0:1, columns])
        staged[h] = (att[h].astype(jnp.float32) * inverse * gain).astype(staged.dtype)
        copy = pltpu.make_async_copy(
            staged.at[h], out_hbm.at[:, pl.ds(h * HEAD_DIM, HEAD_DIM)], out_sem.at[h]
        )
        copy.start()
        copies.append(copy)
    for copy in copies:
        copy.wait()


def on_device(n, queries, keys, values, segment_ids, modality, norm_gain):
    rows, width = queries.shape
    heads = width // HEAD_DIM
    vmem = pl.BlockSpec(memory_space=pltpu.VMEM)
    hbm = pl.BlockSpec(memory_space=pltpu.HBM)
    depth = 2 * rows // PIECES
    block = pltpu.VMEM((heads, PIECES, depth, HEAD_DIM), jnp.bfloat16)
    flow = pltpu.SemaphoreType.DMA((heads, PIECES))
    att, inverse, image = pl.pallas_call(
        functools.partial(kernel, n, heads, rows),
        out_shape=(
            pltpu.VMEM((heads, rows, HEAD_DIM), jnp.bfloat16),
            pltpu.VMEM((rows, HEAD_DIM), jnp.float32),
            pltpu.VMEM((rows, HEAD_DIM), jnp.int32),
        ),
        in_specs=[hbm, hbm, hbm, vmem, vmem],
        out_specs=(vmem, vmem, vmem),
        scratch_shapes=[
            pltpu.VMEM((heads, rows, HEAD_DIM), jnp.bfloat16),
            block,
            block,
            block,
            pltpu.VMEM((1, rows), jnp.int32),
            pltpu.VMEM((1, rows), jnp.int32),
            pltpu.VMEM((rows, (REACH + 1) * rows), jnp.float32),
            pltpu.VMEM((rows, HEAD_DIM), jnp.float32),
            pltpu.VMEM((rows, HEAD_DIM), jnp.float32),
            pltpu.VMEM((rows, HEAD_DIM), jnp.float32),
            pltpu.SemaphoreType.DMA((heads, PIECES + 1)),
            flow,
            flow,
            flow,
            flow,
            flow,
            pltpu.SemaphoreType.DMA((3,)),
            pltpu.SemaphoreType.DMA((2,)),
            pltpu.SemaphoreType.DMA((2,)),
        ],
        compiler_params=pltpu.CompilerParams(
            collective_id=0, has_side_effects=True
        ),
    )(queries, keys, values, segment_ids.reshape(1, rows), modality.reshape(1, rows))
    return pl.pallas_call(
        functools.partial(blend, heads),
        out_shape=jax.ShapeDtypeStruct((rows, width), jnp.bfloat16),
        in_specs=[vmem, vmem, vmem, vmem],
        out_specs=hbm,
        scratch_shapes=[
            pltpu.VMEM((heads, rows, HEAD_DIM), jnp.bfloat16),
            pltpu.SemaphoreType.DMA((heads,)),
        ],
        compiler_params=pltpu.CompilerParams(vmem_limit_bytes=8 * 2**20),
    )(att, inverse, image, norm_gain)


def solution(mesh):
    return jax.shard_map(
        functools.partial(on_device, mesh.shape["seq"]),
        mesh=mesh,
        in_specs=(
            P(("grp", "seq"), "tp"),
            P(("grp", "seq"), "tp"),
            P(("grp", "seq"), "tp"),
            P(("grp", "seq")),
            P(("grp", "seq")),
            P(None, "tp"),
        ),
        out_specs=P(("grp", "seq"), "tp"),
        check_vma=False,
    )
```

```python
import functools

import jax
import jax.numpy as jnp
from jax import lax
from jax.experimental import pallas as pl
from jax.experimental.pallas import tpu as pltpu
from jax.sharding import PartitionSpec as P

HEADS = 16
HEAD_DIM = 128
REACH = 2
MESH = pl.DeviceIdType.MESH
PIECES = 4
DIRECT = 2


def kernel(
    n,
    heads,
    rows,
    q_hbm,
    k_hbm,
    v_hbm,
    seg_ref,
    mod_ref,
    att,
    inverse_ref,
    image_ref,
    q_own,
    own,
    buf1,
    buf2,
    hop,
    seg1,
    seg2,
    bias,
    squares,
    mine,
    theirs,
    in_sem,
    send_a,
    send_b,
    send_c,
    recv_1,
    recv_2,
    hop_recv,
    seg_send,
    seg_recv,
    sq_sem,
):
    s = lax.axis_index("seq")
    t = lax.axis_index("tp")
    even = lax.rem(s, 2) == 0
    odd = lax.rem(s, 2) == 1
    has_next = s + 2 < n
    has_prev = s >= 2
    ahead = odd & (s + 1 < n)
    passes = even & has_next
    behind = even & has_prev
    pair = s + 1 - 2 * lax.rem(s, 2)

    half = PIECES // 2
    depth = rows // half

    def columns_of(h):
        return pl.ds(h * HEAD_DIM, HEAD_DIM)

    def load_piece(h, p):
        source = k_hbm if p < half else v_hbm
        piece = pl.ds((p % half) * depth, depth)
        return pltpu.make_async_copy(
            source.at[piece, columns_of(h)], own.at[h, p], in_sem.at[h, p]
        )

    def load_q(h):
        return pltpu.make_async_copy(q_hbm.at[:, columns_of(h)], q_own.at[h], in_sem.at[h, PIECES])

    last = heads - 1
    direct = range(PIECES - DIRECT, PIECES)
    for p in direct:
        load_piece(last, p).start()
    for h in range(heads):
        for p in range(PIECES):
            if h < last or p not in direct:
                load_piece(h, p).start()

    barrier = pltpu.get_barrier_semaphore()
    pl.semaphore_signal(barrier, inc=1, device_id={"tp": 1 - t}, device_id_type=MESH)
    pl.semaphore_signal(barrier, inc=1, device_id={"seq": pair}, device_id_type=MESH)

    @pl.when(has_next)
    def _():
        pl.semaphore_signal(barrier, inc=1, device_id={"seq": s + 2}, device_id_type=MESH)

    @pl.when(has_prev)
    def _():
        pl.semaphore_signal(barrier, inc=1, device_id={"seq": s - 2}, device_id_type=MESH)

    peers = 2 + jnp.where(has_next, 1, 0) + jnp.where(has_prev, 1, 0)
    pl.semaphore_wait(barrier, peers)

    def remote(source, target, send, recv, where):
        return pltpu.make_async_remote_copy(
            src_ref=source,
            dst_ref=target,
            send_sem=send,
            recv_sem=recv,
            device_id={"seq": where},
            device_id_type=MESH,
        )

    def flow_a(h, p):
        return remote(own.at[h, p], buf1.at[h, p], send_a.at[h, p], recv_1.at[h, p], pair)

    def flow_b(h, p):
        return remote(own.at[h, p], buf2.at[h, p], send_b.at[h, p], recv_2.at[h, p], s + 2)

    def flow_c(h, p):
        return remote(buf2.at[h, p], buf1.at[h, p], send_c.at[h, p], recv_1.at[h, p], pair)

    def flow_d(p):
        i = p - direct[0]
        return remote(own.at[last, p], hop.at[i], send_c.at[last, p], hop_recv.at[i], pair)

    def flow_e(p):
        i = p - direct[0]
        return remote(hop.at[i], buf1.at[last, p], send_c.at[last, p], recv_1.at[last, p], s + 2)

    def forwards(h, p):
        return odd & has_prev & (h < last) if p in direct else odd & has_prev

    def seg_a():
        return remote(seg_ref, seg1, seg_send.at[0], seg_recv.at[0], pair)

    def seg_b():
        return remote(seg_ref, seg2, seg_send.at[1], seg_recv.at[1], s + 2)

    def seg_c():
        return remote(seg2, seg1, seg_send.at[2], seg_recv.at[0], pair)

    @pl.when(even)
    def _():
        seg_a().start()

    @pl.when(has_next)
    def _():
        seg_b().start()

    for p in direct:
        load_piece(last, p).wait()

        @pl.when(ahead)
        def _():
            flow_d(p).start()

    def send_pieces(h, waits):
        for p in range(PIECES):
            if p in waits:
                load_piece(h, p).wait()

            @pl.when(has_next)
            def _():
                flow_b(h, p).start()

            @pl.when(even)
            def _():
                flow_a(h, p).start()

        load_q(h).start()

    def send(h, carry):
        send_pieces(h, range(PIECES))
        return carry

    lax.fori_loop(0, last, send, 0)
    send_pieces(last, range(PIECES - DIRECT))

    @pl.when(s < 1)
    def _():
        buf1[...] = jnp.zeros_like(buf1)
        seg1[...] = jnp.full_like(seg1, -1)

    @pl.when(s < 2)
    def _():
        buf2[...] = jnp.zeros_like(buf2)
        seg2[...] = jnp.full_like(seg2, -1)

    def column(row):
        return jnp.transpose(jnp.broadcast_to(row, (HEAD_DIM, rows)))

    query_seg = column(seg_ref[...])[:, :1]
    query_pos = lax.broadcasted_iota(jnp.int32, (rows, rows), 0)
    key_pos = lax.broadcasted_iota(jnp.int32, (rows, rows), 1)
    allowed = (query_seg == seg_ref[...]) & (key_pos <= query_pos)
    bias[:, :rows] = jnp.where(allowed, 0.0, -jnp.inf)
    squares[...] = jnp.zeros_like(squares)
    image_ref[...] = column(mod_ref[...])

    @pl.when(has_prev)
    def _():
        seg_b().wait_recv()

    @pl.when(odd & has_prev)
    def _():
        seg_c().start()

    @pl.when(s >= 1)
    def _():
        seg_a().wait_recv()

    bias[:, rows : 2 * rows] = jnp.where(query_seg == seg1[...], 0.0, -jnp.inf)
    bias[:, 2 * rows :] = jnp.where(query_seg == seg2[...], 0.0, -jnp.inf)

    for p in direct:

        @pl.when(passes)
        def _():
            flow_d(p).wait_recv()
            flow_e(p).start()

    def scores_of(query, key):
        return lax.dot_general(
            query, key, (((1,), (1,)), ((), ())), preferred_element_type=jnp.float32
        )

    def arrive(h, pieces):
        for p in pieces:

            @pl.when(s >= 1)
            def _():
                flow_a(h, p).wait_recv()

    def head(h, carry):
        load_q(h).wait()
        query = q_own[h]
        scale = HEAD_DIM ** (-0.5)

        def scores_with(block, i):
            key = block[h, :half].reshape(rows, HEAD_DIM)
            return scores_of(query, key) * scale + bias[:, i * rows : (i + 1) * rows]

        def product(weight, block):
            value = block[h, half:].reshape(rows, HEAD_DIM)
            return jnp.dot(
                weight.astype(jnp.bfloat16), value, preferred_element_type=jnp.float32
            )

        for p in range(half):

            @pl.when(has_prev)
            def _():
                flow_b(h, p).wait_recv()

            @pl.when(forwards(h, p))
            def _():
                flow_c(h, p).start()

        @pl.when(odd & has_prev)
        def _():
            for p in range(half, PIECES):
                flow_b(h, p).wait_recv()

                @pl.when(forwards(h, p))
                def _():
                    flow_c(h, p).start()

        near = scores_with(own, 0)
        far = scores_with(buf2, 2)
        arrive(h, range(half))
        middle = scores_with(buf1, 1)
        top = jnp.max(jnp.maximum(jnp.maximum(near, middle), far), axis=1, keepdims=True)
        near = jnp.exp(near - top)
        far = jnp.exp(far - top)
        middle = jnp.exp(middle - top)
        total = jnp.sum(near + middle + far, axis=1, keepdims=True)
        acc = product(near, own)

        @pl.when(behind)
        def _():
            for p in range(half, PIECES):
                flow_b(h, p).wait_recv()

        arrive(h, range(half, PIECES))
        acc = acc + product(far, buf2) + product(middle, buf1)
        attended = (acc * (1.0 / total)).astype(jnp.bfloat16)
        att[h] = attended
        wide = attended.astype(jnp.float32)
        squares[...] += wide * wide
        return carry

    lax.fori_loop(0, heads, head, 0)

    partial = jnp.sum(squares[...], axis=1, keepdims=True)
    mine[...] = jnp.broadcast_to(partial, mine.shape)
    swap = pltpu.make_async_remote_copy(
        src_ref=mine,
        dst_ref=theirs,
        send_sem=sq_sem.at[0],
        recv_sem=sq_sem.at[1],
        device_id={"tp": 1 - t},
        device_id_type=MESH,
    )
    swap.start()
    swap.wait_recv()
    mean_square = (mine[...] + theirs[...]) / (HEADS * HEAD_DIM)
    inverse_ref[...] = lax.rsqrt(mean_square + 1e-05)
    swap.wait_send()

    for p in direct:

        @pl.when(ahead)
        def _():
            flow_d(p).wait_send()

        @pl.when(passes)
        def _():
            flow_e(p).wait_send()

    @pl.when(even)
    def _():
        seg_a().wait_send()

    @pl.when(has_next)
    def _():
        seg_b().wait_send()

    @pl.when(odd & has_prev)
    def _():
        seg_c().wait_send()

    def drain(h, carry):
        for p in range(PIECES):

            @pl.when(even)
            def _():
                flow_a(h, p).wait_send()

            @pl.when(has_next)
            def _():
                flow_b(h, p).wait_send()

            @pl.when(forwards(h, p))
            def _():
                flow_c(h, p).wait_send()

        return carry

    lax.fori_loop(0, heads, drain, 0)


def blend(heads, att, inverse_ref, image_ref, gain_ref, out_hbm, staged, out_sem):
    inverse = inverse_ref[...]
    image = image_ref[...] == 1
    copies = []
    for h in range(heads):
        columns = slice(h * HEAD_DIM, (h + 1) * HEAD_DIM)
        gain = jnp.where(image, gain_ref[1:2, columns], gain_ref[0:1, columns])
        staged[h] = (att[h].astype(jnp.float32) * inverse * gain).astype(staged.dtype)
        copy = pltpu.make_async_copy(
            staged.at[h], out_hbm.at[:, pl.ds(h * HEAD_DIM, HEAD_DIM)], out_sem.at[h]
        )
        copy.start()
        copies.append(copy)
    for copy in copies:
        copy.wait()


def on_device(n, queries, keys, values, segment_ids, modality, norm_gain):
    rows, width = queries.shape
    heads = width // HEAD_DIM
    vmem = pl.BlockSpec(memory_space=pltpu.VMEM)
    hbm = pl.BlockSpec(memory_space=pltpu.HBM)
    depth = 2 * rows // PIECES
    block = pltpu.VMEM((heads, PIECES, depth, HEAD_DIM), jnp.bfloat16)
    flow = pltpu.SemaphoreType.DMA((heads, PIECES))
    att, inverse, image = pl.pallas_call(
        functools.partial(kernel, n, heads, rows),
        out_shape=(
            pltpu.VMEM((heads, rows, HEAD_DIM), jnp.bfloat16),
            pltpu.VMEM((rows, HEAD_DIM), jnp.float32),
            pltpu.VMEM((rows, HEAD_DIM), jnp.int32),
        ),
        in_specs=[hbm, hbm, hbm, vmem, vmem],
        out_specs=(vmem, vmem, vmem),
        scratch_shapes=[
            pltpu.VMEM((heads, rows, HEAD_DIM), jnp.bfloat16),
            block,
            block,
            block,
            pltpu.VMEM((DIRECT, depth, HEAD_DIM), jnp.bfloat16),
            pltpu.VMEM((1, rows), jnp.int32),
            pltpu.VMEM((1, rows), jnp.int32),
            pltpu.VMEM((rows, (REACH + 1) * rows), jnp.float32),
            pltpu.VMEM((rows, HEAD_DIM), jnp.float32),
            pltpu.VMEM((rows, HEAD_DIM), jnp.float32),
            pltpu.VMEM((rows, HEAD_DIM), jnp.float32),
            pltpu.SemaphoreType.DMA((heads, PIECES + 1)),
            flow,
            flow,
            flow,
            flow,
            flow,
            pltpu.SemaphoreType.DMA((DIRECT,)),
            pltpu.SemaphoreType.DMA((3,)),
            pltpu.SemaphoreType.DMA((2,)),
            pltpu.SemaphoreType.DMA((2,)),
        ],
        compiler_params=pltpu.CompilerParams(
            collective_id=0, has_side_effects=True
        ),
    )(queries, keys, values, segment_ids.reshape(1, rows), modality.reshape(1, rows))
    return pl.pallas_call(
        functools.partial(blend, heads),
        out_shape=jax.ShapeDtypeStruct((rows, width), jnp.bfloat16),
        in_specs=[vmem, vmem, vmem, vmem],
        out_specs=hbm,
        scratch_shapes=[
            pltpu.VMEM((heads, rows, HEAD_DIM), jnp.bfloat16),
            pltpu.SemaphoreType.DMA((heads,)),
        ],
        compiler_params=pltpu.CompilerParams(vmem_limit_bytes=8 * 2**20),
    )(att, inverse, image, norm_gain)


def solution(mesh):
    return jax.shard_map(
        functools.partial(on_device, mesh.shape["seq"]),
        mesh=mesh,
        in_specs=(
            P(("grp", "seq"), "tp"),
            P(("grp", "seq"), "tp"),
            P(("grp", "seq"), "tp"),
            P(("grp", "seq")),
            P(("grp", "seq")),
            P(None, "tp"),
        ),
        out_specs=P(("grp", "seq"), "tp"),
        check_vma=False,
    )
```

```python
import functools

import jax
import jax.numpy as jnp
from jax import lax
from jax.experimental import pallas as pl
from jax.experimental.pallas import tpu as pltpu
from jax.sharding import PartitionSpec as P

HEADS = 16
HEAD_DIM = 128
REACH = 2
MESH = pl.DeviceIdType.MESH
PIECES = 4
DIRECT = 2


def kernel(
    n,
    heads,
    rows,
    q_hbm,
    k_hbm,
    v_hbm,
    seg_ref,
    mod_ref,
    att,
    inverse_ref,
    image_ref,
    q_own,
    own,
    buf1,
    buf2,
    hop,
    seg1,
    seg2,
    bias,
    squares,
    mine,
    theirs,
    in_sem,
    send_a,
    send_b,
    send_c,
    recv_1,
    recv_2,
    hop_recv,
    seg_send,
    seg_recv,
    sq_sem,
):
    s = lax.axis_index("seq")
    t = lax.axis_index("tp")
    even = lax.rem(s, 2) == 0
    odd = lax.rem(s, 2) == 1
    has_next = s + 2 < n
    has_prev = s >= 2
    ahead = odd & (s + 1 < n)
    passes = even & has_next
    behind = even & has_prev
    pair = s + 1 - 2 * lax.rem(s, 2)

    half = PIECES // 2
    depth = rows // half

    def columns_of(h):
        return pl.ds(h * HEAD_DIM, HEAD_DIM)

    def load_piece(h, p):
        source = k_hbm if p < half else v_hbm
        piece = pl.ds((p % half) * depth, depth)
        return pltpu.make_async_copy(
            source.at[piece, columns_of(h)], own.at[h, p], in_sem.at[h, p]
        )

    def load_q(h):
        return pltpu.make_async_copy(q_hbm.at[:, columns_of(h)], q_own.at[h], in_sem.at[h, PIECES])

    last = heads - 1
    direct = range(PIECES - DIRECT, PIECES)
    for p in direct:
        load_piece(last, p).start()
    for h in range(heads):
        for p in range(PIECES):
            if h < last or p not in direct:
                load_piece(h, p).start()

    barrier = pltpu.get_barrier_semaphore()
    pl.semaphore_signal(barrier, inc=1, device_id={"tp": 1 - t}, device_id_type=MESH)
    pl.semaphore_signal(barrier, inc=1, device_id={"seq": pair}, device_id_type=MESH)

    @pl.when(has_next)
    def _():
        pl.semaphore_signal(barrier, inc=1, device_id={"seq": s + 2}, device_id_type=MESH)

    @pl.when(has_prev)
    def _():
        pl.semaphore_signal(barrier, inc=1, device_id={"seq": s - 2}, device_id_type=MESH)

    peers = 2 + jnp.where(has_next, 1, 0) + jnp.where(has_prev, 1, 0)
    pl.semaphore_wait(barrier, peers)

    def remote(source, target, send, recv, where):
        return pltpu.make_async_remote_copy(
            src_ref=source,
            dst_ref=target,
            send_sem=send,
            recv_sem=recv,
            device_id={"seq": where},
            device_id_type=MESH,
        )

    def flow_a(h, p):
        return remote(own.at[h, p], buf1.at[h, p], send_a.at[h, p], recv_1.at[h, p], pair)

    def flow_b(h, p):
        return remote(own.at[h, p], buf2.at[h, p], send_b.at[h, p], recv_2.at[h, p], s + 2)

    def flow_c(h, p):
        return remote(buf2.at[h, p], buf1.at[h, p], send_c.at[h, p], recv_1.at[h, p], pair)

    def flow_d(p):
        i = p - direct[0]
        return remote(own.at[last, p], hop.at[i], send_c.at[last, p], hop_recv.at[i], pair)

    def flow_e(p):
        i = p - direct[0]
        return remote(hop.at[i], buf1.at[last, p], send_c.at[last, p], recv_1.at[last, p], s + 2)

    def forwards(h, p):
        return odd & has_prev & (h < last) if p in direct else odd & has_prev

    def seg_a():
        return remote(seg_ref, seg1, seg_send.at[0], seg_recv.at[0], pair)

    def seg_b():
        return remote(seg_ref, seg2, seg_send.at[1], seg_recv.at[1], s + 2)

    def seg_c():
        return remote(seg2, seg1, seg_send.at[2], seg_recv.at[0], pair)

    @pl.when(even)
    def _():
        seg_a().start()

    @pl.when(has_next)
    def _():
        seg_b().start()

    for p in direct:
        load_piece(last, p).wait()

        @pl.when(ahead)
        def _():
            flow_d(p).start()

    def send_pieces(h, waits):
        for p in range(PIECES):
            if p in waits:
                load_piece(h, p).wait()

            @pl.when(has_next)
            def _():
                flow_b(h, p).start()

            @pl.when(even)
            def _():
                flow_a(h, p).start()

        load_q(h).start()

    def send(h, carry):
        send_pieces(h, range(PIECES))
        return carry

    lax.fori_loop(0, last, send, 0)
    send_pieces(last, range(PIECES - DIRECT))

    @pl.when(s < 1)
    def _():
        buf1[...] = jnp.zeros_like(buf1)
        seg1[...] = jnp.full_like(seg1, -1)

    @pl.when(s < 2)
    def _():
        buf2[...] = jnp.zeros_like(buf2)
        seg2[...] = jnp.full_like(seg2, -1)

    def column(row):
        return jnp.transpose(jnp.broadcast_to(row, (HEAD_DIM, rows)))

    query_seg = column(seg_ref[...])[:, :1]
    query_pos = lax.broadcasted_iota(jnp.int32, (rows, rows), 0)
    key_pos = lax.broadcasted_iota(jnp.int32, (rows, rows), 1)
    allowed = (query_seg == seg_ref[...]) & (key_pos <= query_pos)
    bias[:, :rows] = jnp.where(allowed, 0.0, -jnp.inf)
    squares[...] = jnp.zeros_like(squares)
    image_ref[...] = column(mod_ref[...])

    @pl.when(has_prev)
    def _():
        seg_b().wait_recv()

    @pl.when(odd & has_prev)
    def _():
        seg_c().start()

    @pl.when(s >= 1)
    def _():
        seg_a().wait_recv()

    bias[:, rows : 2 * rows] = jnp.where(query_seg == seg1[...], 0.0, -jnp.inf)
    bias[:, 2 * rows :] = jnp.where(query_seg == seg2[...], 0.0, -jnp.inf)

    for p in direct:

        @pl.when(passes)
        def _():
            flow_d(p).wait_recv()
            flow_e(p).start()

    def scores_of(query, key):
        return lax.dot_general(
            query, key, (((1,), (1,)), ((), ())), preferred_element_type=jnp.float32
        )

    def arrive(h, pieces):
        for p in pieces:

            @pl.when(s >= 1)
            def _():
                flow_a(h, p).wait_recv()

    def relay(h, p):
        flow_b(h, p).wait_recv()

        @pl.when(forwards(h, p))
        def _():
            flow_c(h, p).start()

    def relay_next(h, p):
        @pl.when(odd & has_prev & (h < last))
        def _():
            relay(h + 1, p)

    @pl.when(odd & has_prev)
    def _():
        for p in range(PIECES):
            relay(0, p)

    def head(h, carry):
        load_q(h).wait()
        query = q_own[h]
        scale = HEAD_DIM ** (-0.5)

        def scores_with(block, i):
            key = block[h, :half].reshape(rows, HEAD_DIM)
            return scores_of(query, key) * scale + bias[:, i * rows : (i + 1) * rows]

        def product(weight, block):
            value = block[h, half:].reshape(rows, HEAD_DIM)
            return jnp.dot(
                weight.astype(jnp.bfloat16), value, preferred_element_type=jnp.float32
            )

        @pl.when(behind)
        def _():
            for p in range(half):
                flow_b(h, p).wait_recv()

        relay_next(h, 0)
        near = scores_with(own, 0)
        far = scores_with(buf2, 2)
        arrive(h, range(half))
        middle = scores_with(buf1, 1)
        relay_next(h, 1)
        top = jnp.max(jnp.maximum(jnp.maximum(near, middle), far), axis=1, keepdims=True)
        near = jnp.exp(near - top)
        far = jnp.exp(far - top)
        middle = jnp.exp(middle - top)
        total = jnp.sum(near + middle + far, axis=1, keepdims=True)
        relay_next(h, 2)
        acc = product(near, own)

        @pl.when(behind)
        def _():
            for p in range(half, PIECES):
                flow_b(h, p).wait_recv()

        arrive(h, range(half, PIECES))
        acc = acc + product(far, buf2) + product(middle, buf1)
        relay_next(h, 3)
        attended = (acc * (1.0 / total)).astype(jnp.bfloat16)
        att[h] = attended
        wide = attended.astype(jnp.float32)
        squares[...] += wide * wide
        return carry

    lax.fori_loop(0, heads, head, 0)

    partial = jnp.sum(squares[...], axis=1, keepdims=True)
    mine[...] = jnp.broadcast_to(partial, mine.shape)
    swap = pltpu.make_async_remote_copy(
        src_ref=mine,
        dst_ref=theirs,
        send_sem=sq_sem.at[0],
        recv_sem=sq_sem.at[1],
        device_id={"tp": 1 - t},
        device_id_type=MESH,
    )
    swap.start()
    swap.wait_recv()
    mean_square = (mine[...] + theirs[...]) / (HEADS * HEAD_DIM)
    inverse_ref[...] = lax.rsqrt(mean_square + 1e-05)
    swap.wait_send()

    for p in direct:

        @pl.when(ahead)
        def _():
            flow_d(p).wait_send()

        @pl.when(passes)
        def _():
            flow_e(p).wait_send()

    @pl.when(even)
    def _():
        seg_a().wait_send()

    @pl.when(has_next)
    def _():
        seg_b().wait_send()

    @pl.when(odd & has_prev)
    def _():
        seg_c().wait_send()

    def drain(h, carry):
        for p in range(PIECES):

            @pl.when(even)
            def _():
                flow_a(h, p).wait_send()

            @pl.when(has_next)
            def _():
                flow_b(h, p).wait_send()

            @pl.when(forwards(h, p))
            def _():
                flow_c(h, p).wait_send()

        return carry

    lax.fori_loop(0, heads, drain, 0)


def blend(heads, att, inverse_ref, image_ref, gain_ref, out_hbm, staged, out_sem):
    inverse = inverse_ref[...]
    image = image_ref[...] == 1
    copies = []
    for h in range(heads):
        columns = slice(h * HEAD_DIM, (h + 1) * HEAD_DIM)
        gain = jnp.where(image, gain_ref[1:2, columns], gain_ref[0:1, columns])
        staged[h] = (att[h].astype(jnp.float32) * inverse * gain).astype(staged.dtype)
        copy = pltpu.make_async_copy(
            staged.at[h], out_hbm.at[:, pl.ds(h * HEAD_DIM, HEAD_DIM)], out_sem.at[h]
        )
        copy.start()
        copies.append(copy)
    for copy in copies:
        copy.wait()


def on_device(n, queries, keys, values, segment_ids, modality, norm_gain):
    rows, width = queries.shape
    heads = width // HEAD_DIM
    vmem = pl.BlockSpec(memory_space=pltpu.VMEM)
    hbm = pl.BlockSpec(memory_space=pltpu.HBM)
    depth = 2 * rows // PIECES
    block = pltpu.VMEM((heads, PIECES, depth, HEAD_DIM), jnp.bfloat16)
    flow = pltpu.SemaphoreType.DMA((heads, PIECES))
    att, inverse, image = pl.pallas_call(
        functools.partial(kernel, n, heads, rows),
        out_shape=(
            pltpu.VMEM((heads, rows, HEAD_DIM), jnp.bfloat16),
            pltpu.VMEM((rows, HEAD_DIM), jnp.float32),
            pltpu.VMEM((rows, HEAD_DIM), jnp.int32),
        ),
        in_specs=[hbm, hbm, hbm, vmem, vmem],
        out_specs=(vmem, vmem, vmem),
        scratch_shapes=[
            pltpu.VMEM((heads, rows, HEAD_DIM), jnp.bfloat16),
            block,
            block,
            block,
            pltpu.VMEM((DIRECT, depth, HEAD_DIM), jnp.bfloat16),
            pltpu.VMEM((1, rows), jnp.int32),
            pltpu.VMEM((1, rows), jnp.int32),
            pltpu.VMEM((rows, (REACH + 1) * rows), jnp.float32),
            pltpu.VMEM((rows, HEAD_DIM), jnp.float32),
            pltpu.VMEM((rows, HEAD_DIM), jnp.float32),
            pltpu.VMEM((rows, HEAD_DIM), jnp.float32),
            pltpu.SemaphoreType.DMA((heads, PIECES + 1)),
            flow,
            flow,
            flow,
            flow,
            flow,
            pltpu.SemaphoreType.DMA((DIRECT,)),
            pltpu.SemaphoreType.DMA((3,)),
            pltpu.SemaphoreType.DMA((2,)),
            pltpu.SemaphoreType.DMA((2,)),
        ],
        compiler_params=pltpu.CompilerParams(
            collective_id=0, has_side_effects=True
        ),
    )(queries, keys, values, segment_ids.reshape(1, rows), modality.reshape(1, rows))
    return pl.pallas_call(
        functools.partial(blend, heads),
        out_shape=jax.ShapeDtypeStruct((rows, width), jnp.bfloat16),
        in_specs=[vmem, vmem, vmem, vmem],
        out_specs=hbm,
        scratch_shapes=[
            pltpu.VMEM((heads, rows, HEAD_DIM), jnp.bfloat16),
            pltpu.SemaphoreType.DMA((heads,)),
        ],
        compiler_params=pltpu.CompilerParams(vmem_limit_bytes=8 * 2**20),
    )(att, inverse, image, norm_gain)


def solution(mesh):
    return jax.shard_map(
        functools.partial(on_device, mesh.shape["seq"]),
        mesh=mesh,
        in_specs=(
            P(("grp", "seq"), "tp"),
            P(("grp", "seq"), "tp"),
            P(("grp", "seq"), "tp"),
            P(("grp", "seq")),
            P(("grp", "seq")),
            P(None, "tp"),
        ),
        out_specs=P(("grp", "seq"), "tp"),
        check_vma=False,
    )
```

```python
import functools

import jax
import jax.numpy as jnp
from jax import lax
from jax.experimental import pallas as pl
from jax.experimental.pallas import tpu as pltpu
from jax.sharding import PartitionSpec as P

HEADS = 16
HEAD_DIM = 128
REACH = 2
MESH = pl.DeviceIdType.MESH
PIECES = 4
DIRECT = 1


def kernel(
    n,
    heads,
    rows,
    q_hbm,
    k_hbm,
    v_hbm,
    seg_ref,
    mod_ref,
    att,
    inverse_ref,
    image_ref,
    q_own,
    own,
    buf1,
    buf2,
    hop,
    seg1,
    seg2,
    bias,
    squares,
    mine,
    theirs,
    in_sem,
    send_a,
    send_b,
    send_c,
    recv_1,
    recv_2,
    hop_recv,
    seg_send,
    seg_recv,
    sq_sem,
):
    s = lax.axis_index("seq")
    t = lax.axis_index("tp")
    even = lax.rem(s, 2) == 0
    odd = lax.rem(s, 2) == 1
    has_next = s + 2 < n
    has_prev = s >= 2
    ahead = odd & (s + 1 < n)
    passes = even & has_next
    behind = even & has_prev
    pair = s + 1 - 2 * lax.rem(s, 2)

    half = PIECES // 2
    depth = rows // half

    def columns_of(h):
        return pl.ds(h * HEAD_DIM, HEAD_DIM)

    def load_piece(h, p):
        source = k_hbm if p < half else v_hbm
        piece = pl.ds((p % half) * depth, depth)
        return pltpu.make_async_copy(
            source.at[piece, columns_of(h)], own.at[h, p], in_sem.at[h, p]
        )

    def load_q(h):
        return pltpu.make_async_copy(q_hbm.at[:, columns_of(h)], q_own.at[h], in_sem.at[h, PIECES])

    last = heads - 1
    direct = range(PIECES - DIRECT, PIECES)
    for p in direct:
        load_piece(last, p).start()
    for h in range(heads):
        for p in range(PIECES):
            if h < last or p not in direct:
                load_piece(h, p).start()

    barrier = pltpu.get_barrier_semaphore()
    pl.semaphore_signal(barrier, inc=1, device_id={"tp": 1 - t}, device_id_type=MESH)
    pl.semaphore_signal(barrier, inc=1, device_id={"seq": pair}, device_id_type=MESH)

    @pl.when(has_next)
    def _():
        pl.semaphore_signal(barrier, inc=1, device_id={"seq": s + 2}, device_id_type=MESH)

    @pl.when(has_prev)
    def _():
        pl.semaphore_signal(barrier, inc=1, device_id={"seq": s - 2}, device_id_type=MESH)

    peers = 2 + jnp.where(has_next, 1, 0) + jnp.where(has_prev, 1, 0)
    pl.semaphore_wait(barrier, peers)

    def remote(source, target, send, recv, where):
        return pltpu.make_async_remote_copy(
            src_ref=source,
            dst_ref=target,
            send_sem=send,
            recv_sem=recv,
            device_id={"seq": where},
            device_id_type=MESH,
        )

    def flow_a(h, p):
        return remote(own.at[h, p], buf1.at[h, p], send_a.at[h, p], recv_1.at[h, p], pair)

    def flow_b(h, p):
        return remote(own.at[h, p], buf2.at[h, p], send_b.at[h, p], recv_2.at[h, p], s + 2)

    def flow_c(h, p):
        return remote(buf2.at[h, p], buf1.at[h, p], send_c.at[h, p], recv_1.at[h, p], pair)

    def flow_d(p):
        i = p - direct[0]
        return remote(own.at[last, p], hop.at[i], send_c.at[last, p], hop_recv.at[i], pair)

    def flow_e(p):
        i = p - direct[0]
        return remote(hop.at[i], buf1.at[last, p], send_c.at[last, p], recv_1.at[last, p], s + 2)

    def forwards(h, p):
        return odd & has_prev & (h < last) if p in direct else odd & has_prev

    def seg_a():
        return remote(seg_ref, seg1, seg_send.at[0], seg_recv.at[0], pair)

    def seg_b():
        return remote(seg_ref, seg2, seg_send.at[1], seg_recv.at[1], s + 2)

    def seg_c():
        return remote(seg2, seg1, seg_send.at[2], seg_recv.at[0], pair)

    @pl.when(even)
    def _():
        seg_a().start()

    @pl.when(has_next)
    def _():
        seg_b().start()

    for p in direct:
        load_piece(last, p).wait()

        @pl.when(ahead)
        def _():
            flow_d(p).start()

    def send_pieces(h, waits):
        for p in range(PIECES):
            if p in waits:
                load_piece(h, p).wait()

            @pl.when(has_next)
            def _():
                flow_b(h, p).start()

            @pl.when(even)
            def _():
                flow_a(h, p).start()

        load_q(h).start()

    def send(h, carry):
        send_pieces(h, range(PIECES))
        return carry

    lax.fori_loop(0, last, send, 0)
    send_pieces(last, range(PIECES - DIRECT))

    @pl.when(s < 1)
    def _():
        buf1[...] = jnp.zeros_like(buf1)
        seg1[...] = jnp.full_like(seg1, -1)

    @pl.when(s < 2)
    def _():
        buf2[...] = jnp.zeros_like(buf2)
        seg2[...] = jnp.full_like(seg2, -1)

    def column(row):
        return jnp.transpose(jnp.broadcast_to(row, (HEAD_DIM, rows)))

    query_seg = column(seg_ref[...])[:, :1]
    query_pos = lax.broadcasted_iota(jnp.int32, (rows, rows), 0)
    key_pos = lax.broadcasted_iota(jnp.int32, (rows, rows), 1)
    allowed = (query_seg == seg_ref[...]) & (key_pos <= query_pos)
    bias[:, :rows] = jnp.where(allowed, 0.0, -jnp.inf)
    squares[...] = jnp.zeros_like(squares)
    image_ref[...] = column(mod_ref[...])

    @pl.when(has_prev)
    def _():
        seg_b().wait_recv()

    @pl.when(odd & has_prev)
    def _():
        seg_c().start()

    @pl.when(s >= 1)
    def _():
        seg_a().wait_recv()

    bias[:, rows : 2 * rows] = jnp.where(query_seg == seg1[...], 0.0, -jnp.inf)
    bias[:, 2 * rows :] = jnp.where(query_seg == seg2[...], 0.0, -jnp.inf)

    for p in direct:

        @pl.when(passes)
        def _():
            flow_d(p).wait_recv()
            flow_e(p).start()

    def scores_of(query, key):
        return lax.dot_general(
            query, key, (((1,), (1,)), ((), ())), preferred_element_type=jnp.float32
        )

    def arrive(h, pieces):
        for p in pieces:

            @pl.when(s >= 1)
            def _():
                flow_a(h, p).wait_recv()

    def relay(h, p):
        flow_b(h, p).wait_recv()

        @pl.when(forwards(h, p))
        def _():
            flow_c(h, p).start()

    def relay_next(h, p):
        @pl.when(odd & has_prev & (h < last))
        def _():
            relay(h + 1, p)

    @pl.when(odd & has_prev)
    def _():
        for p in range(PIECES):
            relay(0, p)

    def head(h, carry):
        load_q(h).wait()
        query = q_own[h]
        scale = HEAD_DIM ** (-0.5)

        def scores_with(block, i):
            key = block[h, :half].reshape(rows, HEAD_DIM)
            return scores_of(query, key) * scale + bias[:, i * rows : (i + 1) * rows]

        def product(weight, block):
            value = block[h, half:].reshape(rows, HEAD_DIM)
            return jnp.dot(
                weight.astype(jnp.bfloat16), value, preferred_element_type=jnp.float32
            )

        @pl.when(behind)
        def _():
            for p in range(half):
                flow_b(h, p).wait_recv()

        relay_next(h, 0)
        near = scores_with(own, 0)
        far = scores_with(buf2, 2)
        arrive(h, range(half))
        middle = scores_with(buf1, 1)
        relay_next(h, 1)
        top = jnp.max(jnp.maximum(jnp.maximum(near, middle), far), axis=1, keepdims=True)
        near = jnp.exp(near - top)
        far = jnp.exp(far - top)
        middle = jnp.exp(middle - top)
        total = jnp.sum(near + middle + far, axis=1, keepdims=True)
        relay_next(h, 2)
        acc = product(near, own)

        @pl.when(behind)
        def _():
            for p in range(half, PIECES):
                flow_b(h, p).wait_recv()

        arrive(h, range(half, PIECES))
        acc = acc + product(far, buf2) + product(middle, buf1)
        relay_next(h, 3)
        attended = (acc * (1.0 / total)).astype(jnp.bfloat16)
        att[h] = attended
        wide = attended.astype(jnp.float32)
        squares[...] += wide * wide
        return carry

    lax.fori_loop(0, heads, head, 0)

    partial = jnp.sum(squares[...], axis=1, keepdims=True)
    mine[...] = jnp.broadcast_to(partial, mine.shape)
    swap = pltpu.make_async_remote_copy(
        src_ref=mine,
        dst_ref=theirs,
        send_sem=sq_sem.at[0],
        recv_sem=sq_sem.at[1],
        device_id={"tp": 1 - t},
        device_id_type=MESH,
    )
    swap.start()
    swap.wait_recv()
    mean_square = (mine[...] + theirs[...]) / (HEADS * HEAD_DIM)
    inverse_ref[...] = lax.rsqrt(mean_square + 1e-05)
    swap.wait_send()

    for p in direct:

        @pl.when(ahead)
        def _():
            flow_d(p).wait_send()

        @pl.when(passes)
        def _():
            flow_e(p).wait_send()

    @pl.when(even)
    def _():
        seg_a().wait_send()

    @pl.when(has_next)
    def _():
        seg_b().wait_send()

    @pl.when(odd & has_prev)
    def _():
        seg_c().wait_send()

    def drain(h, carry):
        for p in range(PIECES):

            @pl.when(even)
            def _():
                flow_a(h, p).wait_send()

            @pl.when(has_next)
            def _():
                flow_b(h, p).wait_send()

            @pl.when(forwards(h, p))
            def _():
                flow_c(h, p).wait_send()

        return carry

    lax.fori_loop(0, heads, drain, 0)


def blend(heads, att, inverse_ref, image_ref, gain_ref, out_hbm, staged, out_sem):
    inverse = inverse_ref[...]
    image = image_ref[...] == 1
    copies = []
    for h in range(heads):
        columns = slice(h * HEAD_DIM, (h + 1) * HEAD_DIM)
        gain = jnp.where(image, gain_ref[1:2, columns], gain_ref[0:1, columns])
        staged[h] = (att[h].astype(jnp.float32) * inverse * gain).astype(staged.dtype)
        copy = pltpu.make_async_copy(
            staged.at[h], out_hbm.at[:, pl.ds(h * HEAD_DIM, HEAD_DIM)], out_sem.at[h]
        )
        copy.start()
        copies.append(copy)
    for copy in copies:
        copy.wait()


def on_device(n, queries, keys, values, segment_ids, modality, norm_gain):
    rows, width = queries.shape
    heads = width // HEAD_DIM
    vmem = pl.BlockSpec(memory_space=pltpu.VMEM)
    hbm = pl.BlockSpec(memory_space=pltpu.HBM)
    depth = 2 * rows // PIECES
    block = pltpu.VMEM((heads, PIECES, depth, HEAD_DIM), jnp.bfloat16)
    flow = pltpu.SemaphoreType.DMA((heads, PIECES))
    att, inverse, image = pl.pallas_call(
        functools.partial(kernel, n, heads, rows),
        out_shape=(
            pltpu.VMEM((heads, rows, HEAD_DIM), jnp.bfloat16),
            pltpu.VMEM((rows, HEAD_DIM), jnp.float32),
            pltpu.VMEM((rows, HEAD_DIM), jnp.int32),
        ),
        in_specs=[hbm, hbm, hbm, vmem, vmem],
        out_specs=(vmem, vmem, vmem),
        scratch_shapes=[
            pltpu.VMEM((heads, rows, HEAD_DIM), jnp.bfloat16),
            block,
            block,
            block,
            pltpu.VMEM((DIRECT, depth, HEAD_DIM), jnp.bfloat16),
            pltpu.VMEM((1, rows), jnp.int32),
            pltpu.VMEM((1, rows), jnp.int32),
            pltpu.VMEM((rows, (REACH + 1) * rows), jnp.float32),
            pltpu.VMEM((rows, HEAD_DIM), jnp.float32),
            pltpu.VMEM((rows, HEAD_DIM), jnp.float32),
            pltpu.VMEM((rows, HEAD_DIM), jnp.float32),
            pltpu.SemaphoreType.DMA((heads, PIECES + 1)),
            flow,
            flow,
            flow,
            flow,
            flow,
            pltpu.SemaphoreType.DMA((DIRECT,)),
            pltpu.SemaphoreType.DMA((3,)),
            pltpu.SemaphoreType.DMA((2,)),
            pltpu.SemaphoreType.DMA((2,)),
        ],
        compiler_params=pltpu.CompilerParams(
            collective_id=0, has_side_effects=True
        ),
    )(queries, keys, values, segment_ids.reshape(1, rows), modality.reshape(1, rows))
    return pl.pallas_call(
        functools.partial(blend, heads),
        out_shape=jax.ShapeDtypeStruct((rows, width), jnp.bfloat16),
        in_specs=[vmem, vmem, vmem, vmem],
        out_specs=hbm,
        scratch_shapes=[
            pltpu.VMEM((heads, rows, HEAD_DIM), jnp.bfloat16),
            pltpu.SemaphoreType.DMA((heads,)),
        ],
        compiler_params=pltpu.CompilerParams(vmem_limit_bytes=8 * 2**20),
    )(att, inverse, image, norm_gain)


def solution(mesh):
    return jax.shard_map(
        functools.partial(on_device, mesh.shape["seq"]),
        mesh=mesh,
        in_specs=(
            P(("grp", "seq"), "tp"),
            P(("grp", "seq"), "tp"),
            P(("grp", "seq"), "tp"),
            P(("grp", "seq")),
            P(("grp", "seq")),
            P(None, "tp"),
        ),
        out_specs=P(("grp", "seq"), "tp"),
        check_vma=False,
    )
```
